256 devices in a mesh: slab: 128 (over z, x, y), graph: 2 (over core).
Axes of the slice: x: 4, y: 4, z: 8, core: 2. Of those that a mesh axis runs over, the one named last changes fastest.
Arguments:
- nodes: bfloat16 [131072, 9, 128], P(('slab', 'graph')), may hold values from -6 to 6
- boundary: int32 [128, 2, 640], P('slab'), may hold values from 0 to 1023
- sources: int32 [655360], P(('slab', 'graph')), may hold values from 0 to 2303
- targets: int32 [655360], P(('slab', 'graph')), may hold values from 0 to 1023
- block_counts: int32 [128, 2], replicated, may hold values from 10 to 20, as said below
- wigner: float32 [35, 655360], P(None, ('slab', 'graph')), may hold values from -3 to 3
- radial: bfloat16 [655360, 128], P(('slab', 'graph')), may hold values from -6 to 6
- w_zero: bfloat16 [384, 384], replicated, may hold values from -0.3125 to 0.3125
- w_one: bfloat16 [2, 256, 256], replicated, may hold values from -0.25 to 0.25
- w_two: bfloat16 [2, 128, 128], replicated, may hold values from -0.375 to 0.375
Outputs:
- updated: bfloat16 [131072, 9, 128], P(('slab', 'graph'))
The draws below stay inside these ranges and needn't reach their ends.
Inputs may be any that keep to these rules, and one draw needn't show every extreme that they name: Slots of device (s, g) from block_counts[s, g] * 128 on are padding; every draw has some device with 20 live blocks.
All inputs are finite; a program needn't handle non-finite values.
Results may differ from the reference program's by a relative error of at most 0.0064.
Values may be sent and summed in bfloat16 or wider, within the bound.
A program may use at most 64 MiB of HBM per device.

```python
import jax
import jax.numpy as jnp
from jax import lax

CHANNELS = 128
MAX_BLOCKS = 20
EDGE_BLOCK = 128
SLAB_ATOMS = 1024
FACE_ATOMS = 640
TABLE_ROWS = 2304
ATOMS = 131072
EDGES_DEV = 2560
EDGES = 655360
N_SLAB = 128
N_GRAPH = 2


def draw_block_counts(key, part):
    key_counts, key_busiest = jax.random.split(jax.random.fold_in(key, 11))
    least = max(1, MAX_BLOCKS // 2)
    total_devices = N_SLAB * N_GRAPH
    counts = jax.random.randint(key_counts, (total_devices,), least, MAX_BLOCKS + 1, dtype=jnp.int32)
    busiest = jax.random.randint(key_busiest, (), 0, total_devices, dtype=jnp.int32)
    counts = counts.at[busiest].set(MAX_BLOCKS)
    counts = counts.at[(busiest + 1) % total_devices].set(least)
    return counts.reshape(N_SLAB, N_GRAPH)


def with_ends(array, rng, low, high):
    longest = array.shape.index(max(array.shape))
    spots = []
    for shift in (0, 1):
        where = [jax.random.randint(jax.random.fold_in(rng, axis), (), 0, length) for axis, length in enumerate(array.shape)]
        where[longest] = (where[longest] + shift) % array.shape[longest]
        spots.append(tuple(where))
    return array.at[spots[0]].set(low).at[spots[1]].set(high)


def shard_levels(stream_key, dims, cuts, low, top_value):
    factor_of = 1.0
    for axis_at, parts in cuts:
        draws = jax.random.uniform(jax.random.fold_in(jax.random.fold_in(stream_key, 6), axis_at), (parts,), jnp.float32, low / len(cuts), top_value / len(cuts))
        factor_of = factor_of * jnp.repeat(jnp.exp(draws), dims[axis_at] // parts).reshape((-1,) + (1,) * (len(dims) - 1 - axis_at))
    return factor_of


def centred(key, shape, deviation, reach, shards=(), kind=jnp.bfloat16):
    loudness = shard_levels(key, shape, shards, -0.22, 0.18) if shards else 1.0
    entries = jax.random.normal(key, shape, jnp.float32) * deviation * loudness
    return jnp.minimum(jnp.maximum(entries, -reach), reach).astype(kind)


def setup_inputs(seed: int = 0) -> dict:
    key_of = jax.random.split(jax.random.key(seed), 11)
    return {
        "nodes": centred(key_of[0], (ATOMS, 9, CHANNELS), 1.0, 6.0, ((0, 256),)),
        "boundary": with_ends(jax.random.randint(key_of[1], (N_SLAB, 2, FACE_ATOMS), 0, SLAB_ATOMS), jax.random.fold_in(key_of[1], 1), 0, SLAB_ATOMS - 1).astype(jnp.int32),
        "sources": with_ends(jax.random.randint(key_of[2], (EDGES,), 0, TABLE_ROWS), jax.random.fold_in(key_of[2], 1), 0, TABLE_ROWS - 1).astype(jnp.int32),
        "targets": with_ends(jax.random.randint(key_of[3], (EDGES,), 0, SLAB_ATOMS), jax.random.fold_in(key_of[3], 1), 0, SLAB_ATOMS - 1).astype(jnp.int32),
        "block_counts": draw_block_counts(jax.random.fold_in(key_of[10], 71), 0),
        "wigner": centred(key_of[5], (35, EDGES), 0.5, 3.0, ((1, 256),), jnp.float32),
        "radial": centred(key_of[6], (EDGES, CHANNELS), 1.0, 6.0, ((0, 256),)),
        "w_zero": centred(key_of[7], (3 * CHANNELS, 3 * CHANNELS), (3 * CHANNELS) ** -0.5, 0.3125),
        "w_one": centred(key_of[8], (2, 2 * CHANNELS, 2 * CHANNELS), (4 * CHANNELS) ** -0.5, 0.25),
        "w_two": centred(key_of[9], (2, CHANNELS, CHANNELS), (2 * CHANNELS) ** -0.5, 0.375),
    }


message_scale = 0.2
wigner_blocks = ((0, 0, 1), (1, 1, 3), (10, 4, 5))


def rotate(coeffs, wig_rows, inverse):
    out_list = []
    for offset, first_coef, block_size in wigner_blocks:
        for row_index in range(block_size):
            summed = None
            for col_index in range(block_size):
                if inverse:
                    entry_index = offset + col_index * block_size + row_index
                else:
                    entry_index = offset + row_index * block_size + col_index
                product_term = wig_rows[entry_index][:, None] * coeffs[:, first_coef + col_index, :]
                summed = product_term if summed is None else summed + product_term
            out_list.append(summed)
    return jnp.stack(out_list, axis=1)


def build_pair(pair_weights):
    real_part = pair_weights[0]
    imag_part = pair_weights[1]
    top_half = jnp.concatenate([real_part, imag_part], axis=1)
    low_half = jnp.concatenate([-imag_part, real_part], axis=1)
    return jnp.concatenate([top_half, low_half], axis=0)


def mix_orders(rotated, w_zero, pair_one, pair_two):
    chan = rotated.shape[2]
    zero_in = jnp.concatenate([rotated[:, 0], rotated[:, 2], rotated[:, 6]], axis=1)
    zero_out = jnp.dot(zero_in, w_zero, preferred_element_type=jnp.float32)
    one_in = jnp.concatenate([rotated[:, 3], rotated[:, 7], rotated[:, 1], rotated[:, 5]], axis=1)
    one_out = jnp.dot(one_in, pair_one, preferred_element_type=jnp.float32)
    two_in = jnp.concatenate([rotated[:, 8], rotated[:, 4]], axis=1)
    two_out = jnp.dot(two_in, pair_two, preferred_element_type=jnp.float32)
    pieces = [zero_out[:, :chan], one_out[:, 2 * chan:3 * chan], zero_out[:, chan:2 * chan],
              one_out[:, :chan], two_out[:, chan:], one_out[:, 3 * chan:],
              zero_out[:, 2 * chan:], one_out[:, chan:2 * chan], two_out[:, :chan]]
    return jnp.stack(pieces, axis=1).astype(jnp.bfloat16)


def front(src_rows, wig_rows, rad_rows):
    turned = rotate(src_rows.astype(jnp.float32), wig_rows, False)
    return (turned * rad_rows.astype(jnp.float32)[:, None, :]).astype(jnp.bfloat16)


def finish(mixed, wig_rows, live_mask):
    turned = rotate(mixed.astype(jnp.float32), wig_rows, True)
    return (turned * live_mask[:, None, None]).astype(jnp.bfloat16)


def reference(nodes, boundary, sources, targets, block_counts, wigner, radial, w_zero, w_one, w_two):
    pair_one = build_pair(w_one)
    pair_two = build_pair(w_two)
    slabs = nodes.reshape(N_SLAB, SLAB_ATOMS, 9, CHANNELS)
    slots = jnp.arange(EDGES_DEV, dtype=jnp.int32)

    def one_device(totals, device):
        slab_index = device // N_GRAPH
        graph_index = device % N_GRAPH
        below_index = (slab_index + N_SLAB - 1) % N_SLAB
        above_index = (slab_index + 1) % N_SLAB
        lookup = jnp.concatenate([
            slabs[slab_index],
            jnp.take(slabs[below_index], boundary[below_index, 1], axis=0),
            jnp.take(slabs[above_index], boundary[above_index, 0], axis=0)], axis=0)
        begin = (device * EDGES_DEV).astype(jnp.int32)
        src_index = lax.dynamic_slice_in_dim(sources, begin, EDGES_DEV)
        tgt_index = lax.dynamic_slice_in_dim(targets, begin, EDGES_DEV)
        wig_rows = lax.dynamic_slice_in_dim(wigner, begin, EDGES_DEV, 1)
        rad_rows = lax.dynamic_slice_in_dim(radial, begin, EDGES_DEV, 0)
        live_mask = (slots < block_counts[slab_index, graph_index] * EDGE_BLOCK).astype(jnp.float32)
        mixed = mix_orders(front(jnp.take(lookup, src_index, axis=0), wig_rows, rad_rows), w_zero, pair_one, pair_two)
        messages = finish(mixed, wig_rows, live_mask)
        partial_value = jnp.zeros((SLAB_ATOMS, 9 * CHANNELS), jnp.float32).at[tgt_index].add(
            messages.reshape(EDGES_DEV, 9 * CHANNELS).astype(jnp.float32))
        row_start = (slab_index * SLAB_ATOMS).astype(jnp.int32)
        current = lax.dynamic_slice_in_dim(totals, row_start, SLAB_ATOMS, 0)
        return lax.dynamic_update_slice_in_dim(totals, current + partial_value, row_start, 0), None

    initial = jnp.zeros((ATOMS, 9 * CHANNELS), jnp.float32)
    totals, unused = lax.scan(one_device, initial, jnp.arange(N_SLAB * N_GRAPH, dtype=jnp.int32))
    return (totals * message_scale).astype(jnp.bfloat16).reshape(ATOMS, 9, CHANNELS)
```

```python
import jax
import jax.numpy as jnp
from jax import lax
from jax.experimental import pallas as pl
from jax.experimental.pallas import tpu as pltpu
from jax.sharding import PartitionSpec as P

EDGE_BLOCK = 128
ROWS = 9
BLOCKS = ((0, 0, 1), (1, 1, 3), (10, 4, 5))
PLACE = {0: 0, 2: 1, 6: 2, 3: 3, 7: 4, 1: 5, 5: 6, 8: 7, 4: 8}
MESH = pl.DeviceIdType.MESH
message_scale = 0.2
CHUNK = 64


def layer_kernel(
    boundary, src, counts, nodes, tgt, wig, rad, w_zero, w_one, w_two, out,
    table, other, send_up, send_down, from_below, from_above, stage, wscr, spread,
    turned, mixed, msgs, onehot, pair_one, pair_two, sums, arrived,
    n_send, n_recv, up_send, up_recv, down_send, down_recv,
    fb_send, fb_recv, fa_send, fa_recv, s_send, s_recv,
):
    n_slab = lax.axis_size("slab")
    s = lax.axis_index("slab")
    g = lax.axis_index("graph")
    up = lax.rem(s + 1, n_slab)
    down = lax.rem(s + n_slab - 1, n_slab)
    mate = 1 - g
    half = nodes.shape[1]
    slab_atoms = 2 * half
    face = boundary.shape[1]
    mine = face // 2
    edges = src.shape[0]
    chan = nodes.shape[2]
    n_chunk = mine // CHUNK
    crows = CHUNK * ROWS

    barrier = pltpu.get_barrier_semaphore()
    for where in ((s, mate), (up, g), (down, g)):
        pl.semaphore_signal(barrier, inc=1, device_id=where, device_id_type=MESH)
    pl.semaphore_wait(barrier, 3)

    swap = pltpu.make_async_remote_copy(
        src_ref=nodes, dst_ref=other, send_sem=n_send, recv_sem=n_recv,
        device_id=(s, mate), device_id_type=MESH)
    swap.start()

    def fill(planes, first):
        def step(i, _):
            at = pl.multiple_of(i * 16, 16)
            for c in range(ROWS):
                table[pl.ds((first + at) * ROWS + c, 16, stride=ROWS), :] = (
                    planes[c, pl.ds(at, 16), :].astype(jnp.float32))
            return 0
        lax.fori_loop(0, half // 16, step, 0, unroll=2)

    fill(nodes, g * half)

    width = w_one.shape[1]
    pair_one[0:width, 0:width] = w_one[0]
    pair_one[0:width, width:] = w_one[1]
    pair_one[width:, 0:width] = -w_one[1]
    pair_one[width:, width:] = w_one[0]
    pair_two[0:chan, 0:chan] = w_two[0]
    pair_two[0:chan, chan:] = w_two[1]
    pair_two[chan:, 0:chan] = -w_two[1]
    pair_two[chan:, chan:] = w_two[0]
    wscr[...] = jnp.zeros_like(wscr)

    swap.wait()
    fill(other, mate * half)

    def take_rows(row_of, first, count):
        def step(i, _):
            r = row_of(first + i) * ROWS
            stage[pl.ds(i * ROWS, 8), :] = table[pl.ds(r, 8), :]
            stage[pl.ds(i * ROWS + 8, 1), :] = table[pl.ds(r + 8, 1), :]
            return 0
        lax.fori_loop(0, count, step, 0, unroll=16)

    def face_copy(k, buf, dst, ss, rs, to):
        return pltpu.make_async_remote_copy(
            src_ref=buf.at[pl.ds(pl.multiple_of(k * crows, crows), crows), :],
            dst_ref=dst.at[pl.ds(pl.multiple_of((g * n_chunk + k) * crows, crows), crows), :],
            send_sem=ss.at[k], recv_sem=rs.at[k], device_id=(to, g), device_id_type=MESH)

    def send_face(k, _):
        for side, buf, dst, ss, rs, to in (
            (1, send_up, from_below, up_send, up_recv, up),
            (0, send_down, from_above, down_send, down_recv, down)):
            take_rows(lambda i: boundary[side, i], g * mine + k * CHUNK, CHUNK)
            buf[pl.ds(pl.multiple_of(k * crows, crows), crows), :] = (
                stage[0:crows, :].astype(jnp.bfloat16))
            face_copy(k, buf, dst, ss, rs, to).start()
        return 0

    lax.fori_loop(0, n_chunk, send_face, 0)

    live = counts[s, g] * EDGE_BLOCK
    slot = lax.broadcasted_iota(jnp.int32, (1, edges), 1)
    goal = jnp.where(slot < live, tgt[...], -1)

    def mark(i, _):
        at = pl.multiple_of(i * 16, 16)
        first = jnp.where(at < half, mate * half + at, g * half + at - half)
        atom = first + lax.broadcasted_iota(jnp.int32, (16, edges), 0)
        onehot[pl.ds(at, 16), :] = jnp.where(atom == goal, 1.0, 0.0).astype(jnp.bfloat16)
        return 0

    lax.fori_loop(0, slab_atoms // 16, mark, 0)

    def forward(k, buf, ss, rs):
        part = buf.at[pl.ds(pl.multiple_of((g * n_chunk + k) * crows, crows), crows), :]
        return pltpu.make_async_remote_copy(
            src_ref=part, dst_ref=part, send_sem=ss.at[k], recv_sem=rs.at[k],
            device_id=(s, mate), device_id_type=MESH)

    def widen(buf, at, base):
        table[pl.ds(base + at, crows), :] = buf[pl.ds(pl.multiple_of(at, crows), crows), :].astype(jnp.float32)

    sides = (
        (send_up, from_below, up_send, up_recv, up, fb_send, fb_recv, slab_atoms * ROWS),
        (send_down, from_above, down_send, down_recv, down, fa_send, fa_recv, (slab_atoms + face) * ROWS),
    )

    def land(k, _):
        for buf, dst, ss, rs, to, fs, fr, base in sides:
            face_copy(k, buf, dst, ss, rs, to).wait()
            forward(k, dst, fs, fr).start()
            widen(dst, (g * n_chunk + k) * crows, base)
        return 0

    lax.fori_loop(0, n_chunk, land, 0)

    def finish_land(k, _):
        for buf, dst, ss, rs, to, fs, fr, base in sides:
            forward(k, dst, fs, fr).wait()
            widen(dst, (mate * n_chunk + k) * crows, base)
        return 0

    lax.fori_loop(0, n_chunk, finish_land, 0)

    G = 16

    def block(b, _):
        base = pl.multiple_of(b * EDGE_BLOCK, EDGE_BLOCK)
        take_rows(lambda i: src[i], base, EDGE_BLOCK)
        wscr[0:35, :] = wig[:, pl.ds(base, EDGE_BLOCK)]
        wt = wscr[...].T
        for k in range(35):
            spread[k] = jnp.broadcast_to(wt[:, k:k + 1], (EDGE_BLOCK, chan))
        for q in range(EDGE_BLOCK // G):
            rows = slice(q * G, (q + 1) * G)
            rr = rad[pl.ds(base + q * G, G), :].astype(jnp.float32)
            xs = [stage[pl.ds(q * G * ROWS + c, G, stride=ROWS), :] for c in range(ROWS)]
            for off, first, n in BLOCKS:
                for i in range(n):
                    acc = None
                    for j in range(n):
                        term = spread[off + i * n + j, rows, :] * xs[first + j]
                        acc = term if acc is None else acc + term
                    at = PLACE[first + i] * chan
                    turned[rows, at:at + chan] = (acc * rr).astype(jnp.bfloat16)
        mixed[:, 0:3 * chan] = jnp.dot(turned[:, 0:3 * chan], w_zero[...], preferred_element_type=jnp.float32)
        mixed[:, 3 * chan:7 * chan] = jnp.dot(
            turned[:, 3 * chan:7 * chan], pair_one[...], preferred_element_type=jnp.float32)
        mixed[:, 7 * chan:] = jnp.dot(turned[:, 7 * chan:], pair_two[...], preferred_element_type=jnp.float32)
        for q in range(EDGE_BLOCK // G):
            rows = slice(q * G, (q + 1) * G)
            xs = [mixed[rows, PLACE[c] * chan:(PLACE[c] + 1) * chan] for c in range(ROWS)]
            for off, first, n in BLOCKS:
                for i in range(n):
                    acc = None
                    for j in range(n):
                        term = spread[off + j * n + i, rows, :] * xs[first + j]
                        acc = term if acc is None else acc + term
                    c = first + i
                    msgs[c // 2, pl.ds(base + q * G, G), (c % 2) * chan:(c % 2 + 1) * chan] = (
                        acc.astype(jnp.bfloat16))
        return 0

    lax.fori_loop(0, edges // EDGE_BLOCK, block, 0)

    def hand_over(p, w):
        return pltpu.make_async_remote_copy(
            src_ref=sums.at[p, :, pl.ds(0, w)], dst_ref=arrived.at[p, :, pl.ds(0, w)],
            send_sem=s_send.at[p], recv_sem=s_recv.at[p], device_id=(s, mate), device_id_type=MESH)

    widths = [2 * chan] * 4 + [chan]
    for p, w in enumerate(widths):
        sums[p, :, 0:w] = jnp.dot(onehot[0:half, :], msgs[p, :, 0:w], preferred_element_type=jnp.float32)
        hand_over(p, w).start()
    for p, w in enumerate(widths):
        own = jnp.dot(onehot[half:, :], msgs[p, :, 0:w], preferred_element_type=jnp.float32)
        hand_over(p, w).wait()
        total = ((own + arrived[p, :, 0:w]) * message_scale).astype(jnp.bfloat16)
        out[2 * p] = total[:, 0:chan]
        if w > chan:
            out[2 * p + 1] = total[:, chan:]


def per_device(nodes, boundary, sources, targets, block_counts, wigner, radial, w_zero, w_one, w_two):
    half, rows, chan = nodes.shape
    edges = sources.shape[0]
    face = boundary.shape[2]
    n_chunk = face // 2 // CHUNK
    atoms = 2 * half
    vm = pl.BlockSpec(memory_space=pltpu.VMEM)
    sm = pl.BlockSpec(memory_space=pltpu.SMEM)
    dma = pltpu.SemaphoreType.DMA
    out = pl.pallas_call(
        layer_kernel,
        out_shape=jax.ShapeDtypeStruct((rows, half, chan), jnp.bfloat16),
        in_specs=[sm, sm, sm] + [vm] * 7,
        out_specs=vm,
        scratch_shapes=[
            pltpu.VMEM(((atoms + 2 * face) * rows, chan), jnp.float32),
            pltpu.VMEM((rows, half, chan), jnp.bfloat16),
            pltpu.VMEM((face // 2 * rows, chan), jnp.bfloat16),
            pltpu.VMEM((face // 2 * rows, chan), jnp.bfloat16),
            pltpu.VMEM((face * rows, chan), jnp.bfloat16),
            pltpu.VMEM((face * rows, chan), jnp.bfloat16),
            pltpu.VMEM((EDGE_BLOCK * rows, chan), jnp.float32),
            pltpu.VMEM((128, EDGE_BLOCK), jnp.float32),
            pltpu.VMEM((35, EDGE_BLOCK, chan), jnp.float32),
            pltpu.VMEM((EDGE_BLOCK, rows * chan), jnp.bfloat16),
            pltpu.VMEM((EDGE_BLOCK, rows * chan), jnp.float32),
            pltpu.VMEM((5, edges, 2 * chan), jnp.bfloat16),
            pltpu.VMEM((atoms, edges), jnp.bfloat16),
            pltpu.VMEM((4 * chan, 4 * chan), jnp.bfloat16),
            pltpu.VMEM((2 * chan, 2 * chan), jnp.bfloat16),
            pltpu.VMEM((5, half, 2 * chan), jnp.float32),
            pltpu.VMEM((5, half, 2 * chan), jnp.float32),
            dma, dma,
            dma((n_chunk,)), dma((n_chunk,)), dma((n_chunk,)), dma((n_chunk,)),
            dma((n_chunk,)), dma((n_chunk,)), dma((n_chunk,)), dma((n_chunk,)),
            dma((5,)), dma((5,)),
        ],
        compiler_params=pltpu.CompilerParams(
            collective_id=0, has_side_effects=True, vmem_limit_bytes=62 * 1024 * 1024),
        name="layer",
    )(boundary[0], sources, block_counts, jnp.transpose(nodes, (1, 0, 2)), targets[None, :],
      wigner, radial, w_zero, w_one, w_two)
    return jnp.transpose(out, (1, 0, 2))


def solution(mesh):
    return jax.shard_map(
        per_device,
        mesh=mesh,
        in_specs=(
            P(("slab", "graph"), None, None),
            P("slab", None, None),
            P(("slab", "graph")),
            P(("slab", "graph")),
            P(),
            P(None, ("slab", "graph")),
            P(("slab", "graph"), None),
            P(),
            P(),
            P(),
        ),
        out_specs=P(("slab", "graph"), None, None),
        check_vma=False,
    )
```

```python
import functools

import jax
import jax.numpy as jnp
from jax import lax
from jax.experimental import pallas as pl
from jax.experimental.pallas import tpu as pltpu
from jax.sharding import PartitionSpec as P

EDGE_BLOCK = 128
ROWS = 9
BLOCKS = ((0, 0, 1), (1, 1, 3), (10, 4, 5))
PLACE = {0: 0, 2: 1, 6: 2, 3: 3, 7: 4, 1: 5, 5: 6, 8: 7, 4: 8}
MESH = pl.DeviceIdType.MESH
message_scale = 0.2
CHUNK = 64


def weave(*lists):
    items = [((i + 0.5) / len(steps), k, i, step) for k, steps in enumerate(lists) for i, step in enumerate(steps)]
    for item in sorted(items, key=lambda t: t[:3]):
        item[3]()


def layer_kernel(
    boundary, src, counts, nodes, tgt, wig, rad, w_zero, w_one, w_two, out,
    table, other, send_up, send_down, from_below, from_above, stage, across, gain,
    turned, mixed, msgs, onehot, wide_zero, wide_one, wide_two, sums, arrived,
    n_send, n_recv, up_send, up_recv, down_send, down_recv,
    fb_send, fb_recv, fa_send, fa_recv, s_send, s_recv,
):
    n_slab = lax.axis_size("slab")
    s = lax.axis_index("slab")
    g = lax.axis_index("graph")
    up = lax.rem(s + 1, n_slab)
    down = lax.rem(s + n_slab - 1, n_slab)
    mate = 1 - g
    half = nodes.shape[1]
    slab_atoms = 2 * half
    face = boundary.shape[1]
    mine = face // 2
    edges = src.shape[0]
    chan = nodes.shape[2]
    n_chunk = mine // CHUNK
    crows = CHUNK * ROWS

    barrier = pltpu.get_barrier_semaphore()
    for where in ((s, mate), (up, g), (down, g)):
        pl.semaphore_signal(barrier, inc=1, device_id=where, device_id_type=MESH)
    pl.semaphore_wait(barrier, 3)

    swap = pltpu.make_async_remote_copy(
        src_ref=nodes, dst_ref=other, send_sem=n_send, recv_sem=n_recv,
        device_id=(s, mate), device_id_type=MESH)
    swap.start()

    def fill(planes, first):
        def step(i, _):
            at = pl.multiple_of(i * 16, 16)
            for c in range(ROWS):
                table[pl.ds((first + at) * ROWS + c, 16, stride=ROWS), :] = (
                    planes[c, pl.ds(at, 16), :].astype(jnp.float32))
            return 0
        lax.fori_loop(0, half // 16, step, 0, unroll=2)

    fill(nodes, g * half)

    width = w_one.shape[1]
    wide_zero[...] = w_zero[...].T
    real, imag = w_one[0].T, w_one[1].T
    wide_one[0:width, 0:width] = real
    wide_one[0:width, width:] = -imag
    wide_one[width:, 0:width] = imag
    wide_one[width:, width:] = real
    real, imag = w_two[0].T, w_two[1].T
    wide_two[0:chan, 0:chan] = real
    wide_two[0:chan, chan:] = -imag
    wide_two[chan:, 0:chan] = imag
    wide_two[chan:, chan:] = real

    swap.wait()
    fill(other, mate * half)

    def take_row(row, h, i):
        r = row * ROWS
        stage[h, pl.ds(i * ROWS, 8), :] = table[pl.ds(r, 8), :]
        stage[h, pl.ds(i * ROWS + 8, 1), :] = table[pl.ds(r + 8, 1), :]

    def face_copy(k, buf, dst, ss, rs, to):
        return pltpu.make_async_remote_copy(
            src_ref=buf.at[pl.ds(pl.multiple_of(k * crows, crows), crows), :],
            dst_ref=dst.at[pl.ds(pl.multiple_of((g * n_chunk + k) * crows, crows), crows), :],
            send_sem=ss.at[k], recv_sem=rs.at[k], device_id=(to, g), device_id_type=MESH)

    def send_face(k, _):
        for side, buf, dst, ss, rs, to in (
            (1, send_up, from_below, up_send, up_recv, up),
            (0, send_down, from_above, down_send, down_recv, down)):
            def take(i, _):
                take_row(boundary[side, g * mine + k * CHUNK + i], side, i)
                return 0
            lax.fori_loop(0, CHUNK, take, 0, unroll=16)
            buf[pl.ds(pl.multiple_of(k * crows, crows), crows), :] = (
                stage[side, 0:crows, :].astype(jnp.bfloat16))
            face_copy(k, buf, dst, ss, rs, to).start()
        return 0

    lax.fori_loop(0, n_chunk, send_face, 0)

    live = counts[g, s] * EDGE_BLOCK
    slot = lax.broadcasted_iota(jnp.int32, (1, edges), 1)
    goal = jnp.where(slot < live, tgt[...].reshape(1, edges), -1)

    def mark(i, _):
        at = pl.multiple_of(i * 16, 16)
        first = jnp.where(at < half, mate * half + at, g * half + at - half)
        atom = first + lax.broadcasted_iota(jnp.int32, (16, edges), 0)
        onehot[pl.ds(at, 16), :] = jnp.where(atom == goal, 1.0, 0.0).astype(jnp.bfloat16)
        return 0

    lax.fori_loop(0, slab_atoms // 16, mark, 0)

    def forward(k, buf, ss, rs):
        part = buf.at[pl.ds(pl.multiple_of((g * n_chunk + k) * crows, crows), crows), :]
        return pltpu.make_async_remote_copy(
            src_ref=part, dst_ref=part, send_sem=ss.at[k], recv_sem=rs.at[k],
            device_id=(s, mate), device_id_type=MESH)

    def widen(buf, at, base):
        table[pl.ds(base + at, crows), :] = buf[pl.ds(pl.multiple_of(at, crows), crows), :].astype(jnp.float32)

    sides = (
        (send_up, from_below, up_send, up_recv, up, fb_send, fb_recv, slab_atoms * ROWS),
        (send_down, from_above, down_send, down_recv, down, fa_send, fa_recv, (slab_atoms + face) * ROWS),
    )

    def land(k, _):
        for buf, dst, ss, rs, to, fs, fr, base in sides:
            face_copy(k, buf, dst, ss, rs, to).wait()
            forward(k, dst, fs, fr).start()
            widen(dst, (g * n_chunk + k) * crows, base)
        return 0

    lax.fori_loop(0, n_chunk, land, 0)

    def finish_land(k, _):
        for buf, dst, ss, rs, to, fs, fr, base in sides:
            forward(k, dst, fs, fr).wait()
            widen(dst, (mate * n_chunk + k) * crows, base)
        return 0

    lax.fori_loop(0, n_chunk, finish_land, 0)

    G = 16
    lanes = 128
    width = 2 * lanes
    n_block = edges // width

    def gather(base, h):
        def one(i):
            return lambda: take_row(src[base + h * lanes + i], h, i)
        return [one(i) for i in range(lanes)]

    def turn(base, h):
        def one(c):
            def go():
                across[h, c] = stage[h, pl.ds(c, lanes, stride=ROWS), :].T
            return go

        def radial():
            gain[h] = rad[pl.ds(base + h * lanes, lanes), :].astype(jnp.float32).T
        return [one(c) for c in range(ROWS)] + [radial]

    def wide(k, at):
        return jnp.broadcast_to(wig[k:k + 1, pl.ds(at, lanes)], (8, lanes))

    def rotate(base, h, inverse):
        at = base + h * lanes
        cols = slice(h * lanes, (h + 1) * lanes)
        steps = []
        for off, first, n in BLOCKS:
            held = {}

            def go(q, off, first, n, held):
                if q == 0:
                    for k in range(n * n):
                        held[k] = wide(off + k, at)
                tops = (q * G, q * G + 8)
                if inverse:
                    xs = [[mixed[PLACE[first + j] * chan + t:PLACE[first + j] * chan + t + 8, cols] for t in tops]
                          for j in range(n)]
                else:
                    xs = [[across[h, first + j, t:t + 8, :] for t in tops] for j in range(n)]
                    gains = [gain[h, t:t + 8, :] for t in tops]
                for i in range(n):
                    parts = []
                    for u in range(2):
                        acc = None
                        for j in range(n):
                            term = held[j * n + i if inverse else i * n + j] * xs[j][u]
                            acc = term if acc is None else acc + term
                        parts.append(acc if inverse else acc * gains[u])
                    rows = jnp.concatenate(parts, axis=0).astype(jnp.bfloat16)
                    if inverse:
                        top = (first + i) * chan + q * G
                        msgs[top:top + G, pl.ds(at, lanes)] = rows
                    else:
                        top = PLACE[first + i] * chan + q * G
                        turned[top:top + G, cols] = rows

            for q in range(chan // G):
                steps.append(functools.partial(go, q, off, first, n, held))
        return steps

    def mixing():
        for lo, hi, w in ((3, 7, wide_one), (0, 3, wide_zero), (7, 9, wide_two)):
            mixed[lo * chan:hi * chan, :] = jnp.dot(
                w[...], turned[lo * chan:hi * chan, :], preferred_element_type=jnp.float32)

    for h in range(2):
        weave(gather(0, h))
        weave(turn(0, h))

    def block(b, _):
        base = pl.multiple_of(b * width, width)
        after = pl.multiple_of(jnp.where(b + 1 < n_block, b + 1, 0) * width, width)
        weave(rotate(base, 0, False), gather(after, 0))
        weave(rotate(base, 1, False), gather(after, 1), turn(after, 0))
        mixing()
        weave(rotate(base, 0, True) + rotate(base, 1, True), turn(after, 1))
        return 0

    lax.fori_loop(0, n_block, block, 0)

    def hand_over(p, w):
        return pltpu.make_async_remote_copy(
            src_ref=sums.at[p, :, pl.ds(0, w)], dst_ref=arrived.at[p, :, pl.ds(0, w)],
            send_sem=s_send.at[p], recv_sem=s_recv.at[p], device_id=(s, mate), device_id_type=MESH)

    def total_of(lo, hi, p, w):
        return lax.dot_general(
            onehot[lo:hi, :], msgs[p * 2 * chan:p * 2 * chan + w, :], (((1,), (1,)), ((), ())),
            preferred_element_type=jnp.float32)

    widths = [2 * chan] * 4 + [chan]
    for p, w in enumerate(widths):
        sums[p, :, 0:w] = total_of(0, half, p, w)
        hand_over(p, w).start()
    for p, w in enumerate(widths):
        own = total_of(half, 2 * half, p, w)
        hand_over(p, w).wait()
        total = ((own + arrived[p, :, 0:w]) * message_scale).astype(jnp.bfloat16)
        out[2 * p] = total[:, 0:chan]
        if w > chan:
            out[2 * p + 1] = total[:, chan:]


def per_device(nodes, boundary, sources, targets, block_counts, wigner, radial, w_zero, w_one, w_two):
    half, rows, chan = nodes.shape
    edges = sources.shape[0]
    face = boundary.shape[2]
    n_chunk = face // 2 // CHUNK
    atoms = 2 * half
    vm = pl.BlockSpec(memory_space=pltpu.VMEM)
    sm = pl.BlockSpec(memory_space=pltpu.SMEM)
    dma = pltpu.SemaphoreType.DMA
    out = pl.pallas_call(
        layer_kernel,
        out_shape=jax.ShapeDtypeStruct((rows, half, chan), jnp.bfloat16),
        in_specs=[sm, sm, sm] + [vm] * 7,
        out_specs=vm,
        scratch_shapes=[
            pltpu.VMEM(((atoms + 2 * face) * rows, chan), jnp.float32),
            pltpu.VMEM((rows, half, chan), jnp.bfloat16),
            pltpu.VMEM((face // 2 * rows, chan), jnp.bfloat16),
            pltpu.VMEM((face // 2 * rows, chan), jnp.bfloat16),
            pltpu.VMEM((face * rows, chan), jnp.bfloat16),
            pltpu.VMEM((face * rows, chan), jnp.bfloat16),
            pltpu.VMEM((2, 128 * rows, chan), jnp.float32),
            pltpu.VMEM((2, rows, chan, 128), jnp.float32),
            pltpu.VMEM((2, chan, 128), jnp.float32),
            pltpu.VMEM((rows * chan, 256), jnp.bfloat16),
            pltpu.VMEM((rows * chan, 256), jnp.float32),
            pltpu.VMEM((rows * chan, edges), jnp.bfloat16),
            pltpu.VMEM((atoms, edges), jnp.bfloat16),
            pltpu.VMEM((3 * chan, 3 * chan), jnp.bfloat16),
            pltpu.VMEM((4 * chan, 4 * chan), jnp.bfloat16),
            pltpu.VMEM((2 * chan, 2 * chan), jnp.bfloat16),
            pltpu.VMEM((5, half, 2 * chan), jnp.float32),
            pltpu.VMEM((5, half, 2 * chan), jnp.float32),
            dma, dma,
            dma((n_chunk,)), dma((n_chunk,)), dma((n_chunk,)), dma((n_chunk,)),
            dma((n_chunk,)), dma((n_chunk,)), dma((n_chunk,)), dma((n_chunk,)),
            dma((5,)), dma((5,)),
        ],
        compiler_params=pltpu.CompilerParams(
            collective_id=0, has_side_effects=True, vmem_limit_bytes=62 * 1024 * 1024),
        name="layer",
    )(boundary[0], sources, block_counts.T, jnp.transpose(nodes, (1, 0, 2)), targets,
      wigner, radial, w_zero, w_one, w_two)
    return jnp.transpose(out, (1, 0, 2))


def solution(mesh):
    return jax.shard_map(
        per_device,
        mesh=mesh,
        in_specs=(
            P(("slab", "graph"), None, None),
            P("slab", None, None),
            P(("slab", "graph")),
            P(("slab", "graph")),
            P(),
            P(None, ("slab", "graph")),
            P(("slab", "graph"), None),
            P(),
            P(),
            P(),
        ),
        out_specs=P(("slab", "graph"), None, None),
        check_vma=False,
    )
```

```python
import functools

import jax
import jax.numpy as jnp
from jax import lax
from jax.experimental import pallas as pl
from jax.experimental.pallas import tpu as pltpu
from jax.sharding import PartitionSpec as P

EDGE_BLOCK = 128
ROWS = 9
BLOCKS = ((0, 0, 1), (1, 1, 3), (10, 4, 5))
PLACE = {0: 0, 2: 1, 6: 2, 3: 3, 7: 4, 1: 5, 5: 6, 8: 7, 4: 8}
MESH = pl.DeviceIdType.MESH
message_scale = 0.2
CHUNK = 32


def weave(*lists):
    items = [((i + 0.5) / len(steps), k, i, step) for k, steps in enumerate(lists) for i, step in enumerate(steps)]
    for item in sorted(items, key=lambda t: t[:3]):
        item[3]()


def layer_kernel(
    boundary_hbm, src_hbm, counts_hbm, nodes_hbm, tgt_hbm, wig_hbm, rad_hbm, zero_hbm, one_hbm, two_hbm, out,
    boundary, src, counts, nodes, tgt, wig, rad, w_zero, w_one, w_two, local_sem,
    table, other, send_up, send_down, from_below, from_above, stage, across, gain, spread,
    turned, mixed, msgs, onehot, goal, wide_zero, wide_one, wide_two, sums, leaving, arrived,
    n_send, n_recv, up_send, up_recv, down_send, down_recv,
    fb_send, fb_recv, fa_send, fa_recv, s_send, s_recv,
):
    n_slab = lax.axis_size("slab")
    s = lax.axis_index("slab")
    g = lax.axis_index("graph")
    up = lax.rem(s + 1, n_slab)
    down = lax.rem(s + n_slab - 1, n_slab)
    mate = 1 - g
    half = nodes.shape[1]
    slab_atoms = 2 * half
    face = boundary.shape[1]
    mine = face // 2
    edges = src.shape[0]
    chan = nodes.shape[2]
    n_chunk = mine // CHUNK
    crows = CHUNK * ROWS

    local = [
        pltpu.make_async_copy(a, b, local_sem.at[i])
        for i, (a, b) in enumerate((
            (nodes_hbm, nodes), (boundary_hbm, boundary), (zero_hbm, w_zero), (one_hbm, w_one), (two_hbm, w_two),
            (counts_hbm, counts), (tgt_hbm, tgt), (src_hbm, src), (wig_hbm, wig), (rad_hbm, rad)))]
    for copy in local:
        copy.start()

    barrier = pltpu.get_barrier_semaphore()
    for where in ((s, mate), (up, g), (down, g)):
        pl.semaphore_signal(barrier, inc=1, device_id=where, device_id_type=MESH)
    pl.semaphore_wait(barrier, 3)

    swap = pltpu.make_async_remote_copy(
        src_ref=nodes_hbm, dst_ref=other, send_sem=n_send, recv_sem=n_recv,
        device_id=(s, mate), device_id_type=MESH)
    swap.start()

    def fill(planes, first):
        def step(i, _):
            at = pl.multiple_of(i * 16, 16)
            for c in range(ROWS):
                table[pl.ds((first + at) * ROWS + c, 16, stride=ROWS), :] = (
                    planes[c, pl.ds(at, 16), :].astype(jnp.float32))
            return 0
        lax.fori_loop(0, half // 16, step, 0, unroll=2)

    local[0].wait()
    fill(nodes, g * half)
    for copy in local[1:5]:
        copy.wait()

    width = w_one.shape[1]
    wide_zero[...] = w_zero[...].T
    real, imag = w_one[0].T, w_one[1].T
    wide_one[0:width, 0:width] = real
    wide_one[0:width, width:] = -imag
    wide_one[width:, 0:width] = imag
    wide_one[width:, width:] = real
    real, imag = w_two[0].T, w_two[1].T
    wide_two[0:chan, 0:chan] = real
    wide_two[0:chan, chan:] = -imag
    wide_two[chan:, 0:chan] = imag
    wide_two[chan:, chan:] = real

    swap.wait()
    fill(other, mate * half)

    def take_row(row, h, i):
        r = row * ROWS
        stage[h, pl.ds(i * ROWS, 8), :] = table[pl.ds(r, 8), :]
        stage[h, pl.ds(i * ROWS + 8, 1), :] = table[pl.ds(r + 8, 1), :]

    def face_copy(k, buf, dst, ss, rs, to):
        return pltpu.make_async_remote_copy(
            src_ref=buf.at[pl.ds(pl.multiple_of(k * crows, crows), crows), :],
            dst_ref=dst.at[pl.ds(pl.multiple_of((g * n_chunk + k) * crows, crows), crows), :],
            send_sem=ss.at[k], recv_sem=rs.at[k], device_id=(to, g), device_id_type=MESH)

    def send_face(k, _):
        for side, buf, dst, ss, rs, to in (
            (1, send_up, from_below, up_send, up_recv, up),
            (0, send_down, from_above, down_send, down_recv, down)):
            def take(i, _):
                take_row(boundary[side, g * mine + k * CHUNK + i], side, i)
                return 0
            lax.fori_loop(0, CHUNK, take, 0, unroll=16)
            buf[pl.ds(pl.multiple_of(k * crows, crows), crows), :] = (
                stage[side, 0:crows, :].astype(jnp.bfloat16))
            face_copy(k, buf, dst, ss, rs, to).start()
        return 0

    lax.fori_loop(0, n_chunk, send_face, 0)

    for copy in local[5:]:
        copy.wait()

    live = counts[g, s] * EDGE_BLOCK
    slot = lax.broadcasted_iota(jnp.int32, (1, edges), 1)
    goal[...] = jnp.where(slot < live, tgt[...].reshape(1, edges), -1)
    atom = lax.broadcasted_iota(jnp.int32, (128, half), 1)

    def mark(i, _):
        at = pl.multiple_of(i * 128, 128)
        aim = jnp.broadcast_to(goal[:, pl.ds(at, 128)], (128, 128)).T
        aim = jnp.concatenate([aim] * (half // 128), axis=1)
        for k, who in enumerate((mate, g)):
            onehot[k, pl.ds(at, 128), :] = jnp.where(aim == atom + who * half, 1.0, 0.0).astype(jnp.bfloat16)
        return 0

    lax.fori_loop(0, edges // 128, mark, 0)

    def clear(i, _):
        for k in range(2):
            sums[k, pl.ds(pl.multiple_of(i * 32, 32), 32), :] = jnp.zeros((32, half), jnp.float32)
        return 0

    lax.fori_loop(0, ROWS * chan // 32, clear, 0)
    msgs[:, edges - 512:] = jnp.zeros((ROWS * chan, 512), jnp.bfloat16)

    def forward(k, buf, ss, rs):
        part = buf.at[pl.ds(pl.multiple_of((g * n_chunk + k) * crows, crows), crows), :]
        return pltpu.make_async_remote_copy(
            src_ref=part, dst_ref=part, send_sem=ss.at[k], recv_sem=rs.at[k],
            device_id=(s, mate), device_id_type=MESH)

    def widen(buf, at, base):
        table[pl.ds(base + at, crows), :] = buf[pl.ds(pl.multiple_of(at, crows), crows), :].astype(jnp.float32)

    sides = (
        (send_up, from_below, up_send, up_recv, up, fb_send, fb_recv, slab_atoms * ROWS),
        (send_down, from_above, down_send, down_recv, down, fa_send, fa_recv, (slab_atoms + face) * ROWS),
    )

    def land(k, _):
        for buf, dst, ss, rs, to, fs, fr, base in sides:
            face_copy(k, buf, dst, ss, rs, to).wait()
            forward(k, dst, fs, fr).start()
            widen(dst, (g * n_chunk + k) * crows, base)
        return 0

    lax.fori_loop(0, n_chunk, land, 0)

    def finish_land(k, _):
        for buf, dst, ss, rs, to, fs, fr, base in sides:
            forward(k, dst, fs, fr).wait()
            widen(dst, (mate * n_chunk + k) * crows, base)
        return 0

    lax.fori_loop(0, n_chunk, finish_land, 0)

    G = 32
    lanes = 128
    width = 2 * lanes
    n_block = edges // width

    def gather(base, h):
        def one(i):
            return lambda: take_row(src[base + h * lanes + i], h, i)
        return [one(i) for i in range(lanes)]

    def turn(base, h):
        def one(c):
            def go():
                across[h, c] = stage[h, pl.ds(c, lanes, stride=ROWS), :].T
            return go

        def radial():
            gain[h] = rad[pl.ds(base + h * lanes, lanes), :].astype(jnp.float32).T
        return [one(c) for c in range(ROWS)] + [radial]

    def widen_rows(base, h):
        def go():
            for k in range(wig.shape[0]):
                spread[h, k] = jnp.broadcast_to(wig[k:k + 1, pl.ds(base + h * lanes, lanes)], (8, lanes))
        return [go]

    def rotate(base, h, inverse):
        at = base + h * lanes
        cols = slice(h * lanes, (h + 1) * lanes)
        steps = []
        for off, first, n in BLOCKS:

            def go(q, off, first, n):
                tops = range(q * G, (q + 1) * G, 8)
                if inverse:
                    xs = [[mixed[PLACE[first + j] * chan + t:PLACE[first + j] * chan + t + 8, cols] for t in tops]
                          for j in range(n)]
                else:
                    xs = [[across[h, first + j, t:t + 8, :] for t in tops] for j in range(n)]
                    gains = [gain[h, t:t + 8, :] for t in tops]
                for i in range(n):
                    parts = []
                    for u in range(len(tops)):
                        acc = None
                        for j in range(n):
                            term = spread[h, off + (j * n + i if inverse else i * n + j)] * xs[j][u]
                            acc = term if acc is None else acc + term
                        parts.append(acc if inverse else acc * gains[u])
                    rows = jnp.concatenate(parts, axis=0).astype(jnp.bfloat16)
                    if inverse:
                        top = (first + i) * chan + q * G
                        msgs[top:top + G, pl.ds(at, lanes)] = rows
                    else:
                        top = PLACE[first + i] * chan + q * G
                        turned[top:top + G, cols] = rows

            for q in range(chan // G):
                steps.append(functools.partial(go, q, off, first, n))
        return steps

    def mixing():
        for lo, hi, w in ((3, 7, wide_one), (0, 3, wide_zero), (7, 9, wide_two)):
            mixed[lo * chan:hi * chan, :] = jnp.dot(
                w[...], turned[lo * chan:hi * chan, :], preferred_element_type=jnp.float32)

    for h in range(2):
        weave(gather(0, h))
        weave(turn(0, h))

    span = 2 * width

    def add_up(side, pair):
        cols = pl.ds(pl.multiple_of(pair * span, span), span)

        def one(p):
            def go():
                atoms = slice(p * 256, (p + 1) * 256)
                sums[side, :, atoms] += jnp.dot(
                    msgs[:, cols], onehot[side, cols, atoms], preferred_element_type=jnp.float32)
            return go
        return [one(p) for p in range(half // 256)]

    def block(b, _):
        base = pl.multiple_of(b * width, width)
        pair = jnp.where(b < 2, n_block // 2 - 1, b // 2 - 1)
        adds = add_up(lax.rem(b, 2), pair)
        after = pl.multiple_of(jnp.where(b + 1 < n_block, b + 1, 0) * width, width)
        weave(widen_rows(base, 0))
        weave(widen_rows(base, 1))
        weave(rotate(base, 0, False), gather(after, 0), adds[0:1])
        weave(rotate(base, 1, False), gather(after, 1), turn(after, 0), adds[1:2])
        mixing()
        weave(turn(after, 1))
        weave(rotate(base, 0, True))
        weave(rotate(base, 1, True))
        return 0

    lax.fori_loop(0, n_block, block, 0)

    part = 3 * chan

    def hand_over(p):
        return pltpu.make_async_remote_copy(
            src_ref=leaving.at[p], dst_ref=arrived.at[p],
            send_sem=s_send.at[p], recv_sem=s_recv.at[p], device_id=(s, mate), device_id_type=MESH)

    last = n_block // 2 - 1
    weave(add_up(0, last))
    for p in range(3):
        leaving[p] = sums[0, p * part:(p + 1) * part, :].astype(jnp.bfloat16)
        hand_over(p).start()
    weave(add_up(1, last))
    for p in range(3):
        hand_over(p).wait()
        total = sums[1, p * part:(p + 1) * part, :] + arrived[p].astype(jnp.float32)
        total = (total * message_scale).astype(jnp.bfloat16)
        for c in range(3):
            out[3 * p + c] = total[c * chan:(c + 1) * chan, :].T


def per_device(nodes, boundary, sources, targets, block_counts, wigner, radial, w_zero, w_one, w_two):
    half, rows, chan = nodes.shape
    edges = sources.shape[0]
    face = boundary.shape[2]
    n_chunk = face // 2 // CHUNK
    atoms = 2 * half
    vm = pl.BlockSpec(memory_space=pltpu.VMEM)
    hbm = pl.BlockSpec(memory_space=pltpu.HBM)
    dma = pltpu.SemaphoreType.DMA
    out = pl.pallas_call(
        layer_kernel,
        out_shape=jax.ShapeDtypeStruct((rows, half, chan), jnp.bfloat16),
        in_specs=[hbm] * 10,
        out_specs=vm,
        scratch_shapes=[
            pltpu.SMEM((2, face), jnp.int32),
            pltpu.SMEM((edges,), jnp.int32),
            pltpu.SMEM(block_counts.shape[::-1], jnp.int32),
            pltpu.VMEM((rows, half, chan), jnp.bfloat16),
            pltpu.VMEM((edges,), jnp.int32),
            pltpu.VMEM(wigner.shape, jnp.float32),
            pltpu.VMEM(radial.shape, jnp.bfloat16),
            pltpu.VMEM(w_zero.shape, jnp.bfloat16),
            pltpu.VMEM(w_one.shape, jnp.bfloat16),
            pltpu.VMEM(w_two.shape, jnp.bfloat16),
            dma((10,)),
            pltpu.VMEM(((atoms + 2 * face) * rows, chan), jnp.float32),
            pltpu.VMEM((rows, half, chan), jnp.bfloat16),
            pltpu.VMEM((face // 2 * rows, chan), jnp.bfloat16),
            pltpu.VMEM((face // 2 * rows, chan), jnp.bfloat16),
            pltpu.VMEM((face * rows, chan), jnp.bfloat16),
            pltpu.VMEM((face * rows, chan), jnp.bfloat16),
            pltpu.VMEM((2, 128 * rows, chan), jnp.float32),
            pltpu.VMEM((2, rows, chan, 128), jnp.float32),
            pltpu.VMEM((2, chan, 128), jnp.float32),
            pltpu.VMEM((2, 35, 8, 128), jnp.float32),
            pltpu.VMEM((rows * chan, 256), jnp.bfloat16),
            pltpu.VMEM((rows * chan, 256), jnp.float32),
            pltpu.VMEM((rows * chan, edges), jnp.bfloat16),
            pltpu.VMEM((2, edges, half), jnp.bfloat16),
            pltpu.VMEM((1, edges), jnp.int32),
            pltpu.VMEM((3 * chan, 3 * chan), jnp.bfloat16),
            pltpu.VMEM((4 * chan, 4 * chan), jnp.bfloat16),
            pltpu.VMEM((2 * chan, 2 * chan), jnp.bfloat16),
            pltpu.VMEM((2, rows * chan, half), jnp.float32),
            pltpu.VMEM((3, 3 * chan, half), jnp.bfloat16),
            pltpu.VMEM((3, 3 * chan, half), jnp.bfloat16),
            dma, dma,
            dma((n_chunk,)), dma((n_chunk,)), dma((n_chunk,)), dma((n_chunk,)),
            dma((n_chunk,)), dma((n_chunk,)), dma((n_chunk,)), dma((n_chunk,)),
            dma((3,)), dma((3,)),
        ],
        compiler_params=pltpu.CompilerParams(
            collective_id=0, has_side_effects=True, vmem_limit_bytes=62 * 1024 * 1024),
        name="layer",
    )(boundary[0], sources, block_counts.T, jnp.transpose(nodes, (1, 0, 2)), targets,
      wigner, radial, w_zero, w_one, w_two)
    return jnp.transpose(out, (1, 0, 2))


def solution(mesh):
    return jax.shard_map(
        per_device,
        mesh=mesh,
        in_specs=(
            P(("slab", "graph"), None, None),
            P("slab", None, None),
            P(("slab", "graph")),
            P(("slab", "graph")),
            P(),
            P(None, ("slab", "graph")),
            P(("slab", "graph"), None),
            P(),
            P(),
            P(),
        ),
        out_specs=P(("slab", "graph"), None, None),
        check_vma=False,
    )
```

```python
import functools

import jax
import jax.numpy as jnp
from jax import lax
from jax.experimental import pallas as pl
from jax.experimental.pallas import tpu as pltpu
from jax.sharding import PartitionSpec as P

EDGE_BLOCK = 128
ROWS = 9
BLOCKS = ((0, 0, 1), (1, 1, 3), (10, 4, 5))
PLACE = {0: 0, 2: 1, 6: 2, 3: 3, 7: 4, 1: 5, 5: 6, 8: 7, 4: 8}
MESH = pl.DeviceIdType.MESH
message_scale = 0.2
CHUNK = 32


def weave(*lists):
    items = [((i + 0.5) / len(steps), k, i, step) for k, steps in enumerate(lists) for i, step in enumerate(steps)]
    for item in sorted(items, key=lambda t: t[:3]):
        item[3]()


def layer_kernel(
    boundary_hbm, src_hbm, counts_hbm, nodes_hbm, tgt_hbm, wig_hbm, rad_hbm, zero_hbm, one_hbm, two_hbm, out,
    boundary, src, counts, nodes, tgt, wig, rad, w_zero, w_one, w_two, local_sem,
    table, other, send_up, send_down, from_below, from_above, stage, across, gain, spread,
    turned, mixed, msgs, onehot, goal, wide_zero, wide_one, wide_two, sums, leaving, arrived,
    n_send, n_recv, up_send, up_recv, down_send, down_recv,
    fb_send, fb_recv, fa_send, fa_recv, s_send, s_recv,
):
    n_slab = lax.axis_size("slab")
    s = lax.axis_index("slab")
    g = lax.axis_index("graph")
    up = lax.rem(s + 1, n_slab)
    down = lax.rem(s + n_slab - 1, n_slab)
    mate = 1 - g
    half = nodes.shape[1]
    slab_atoms = 2 * half
    face = boundary.shape[1]
    mine = face // 2
    edges = src.shape[0]
    chan = nodes.shape[2]
    n_chunk = mine // CHUNK
    crows = CHUNK * ROWS

    local = [
        pltpu.make_async_copy(a, b, local_sem.at[i])
        for i, (a, b) in enumerate((
            (nodes_hbm, nodes), (boundary_hbm, boundary), (zero_hbm, w_zero), (one_hbm, w_one), (two_hbm, w_two),
            (counts_hbm, counts), (tgt_hbm, tgt), (src_hbm, src), (wig_hbm, wig), (rad_hbm, rad)))]
    for copy in local:
        copy.start()

    barrier = pltpu.get_barrier_semaphore()
    for where in ((s, mate), (up, g), (down, g)):
        pl.semaphore_signal(barrier, inc=1, device_id=where, device_id_type=MESH)
    pl.semaphore_wait(barrier, 3)

    swap = pltpu.make_async_remote_copy(
        src_ref=nodes_hbm, dst_ref=other, send_sem=n_send, recv_sem=n_recv,
        device_id=(s, mate), device_id_type=MESH)
    swap.start()

    def fill(planes, first):
        def step(i, _):
            at = pl.multiple_of(i * 16, 16)
            for c in range(ROWS):
                table[pl.ds((first + at) * ROWS + c, 16, stride=ROWS), :] = (
                    planes[c, pl.ds(at, 16), :].astype(jnp.float32))
            return 0
        lax.fori_loop(0, half // 16, step, 0, unroll=2)

    local[0].wait()
    fill(nodes, g * half)
    for copy in local[1:5]:
        copy.wait()

    width = w_one.shape[1]
    wide_zero[...] = w_zero[...].T
    real, imag = w_one[0].T, w_one[1].T
    wide_one[0:width, 0:width] = real
    wide_one[0:width, width:] = -imag
    wide_one[width:, 0:width] = imag
    wide_one[width:, width:] = real
    real, imag = w_two[0].T, w_two[1].T
    wide_two[0:chan, 0:chan] = real
    wide_two[0:chan, chan:] = -imag
    wide_two[chan:, 0:chan] = imag
    wide_two[chan:, chan:] = real

    swap.wait()
    fill(other, mate * half)

    def take_row(row, h, i):
        r = row * ROWS
        stage[h, pl.ds(i * ROWS, 8), :] = table[pl.ds(r, 8), :]
        stage[h, pl.ds(i * ROWS + 8, 1), :] = table[pl.ds(r + 8, 1), :]

    def face_copy(k, buf, dst, ss, rs, to):
        return pltpu.make_async_remote_copy(
            src_ref=buf.at[pl.ds(pl.multiple_of(k * crows, crows), crows), :],
            dst_ref=dst.at[pl.ds(pl.multiple_of((g * n_chunk + k) * crows, crows), crows), :],
            send_sem=ss.at[k], recv_sem=rs.at[k], device_id=(to, g), device_id_type=MESH)

    def send_face(k, _):
        for side, buf, dst, ss, rs, to in (
            (1, send_up, from_below, up_send, up_recv, up),
            (0, send_down, from_above, down_send, down_recv, down)):
            def take(i, _):
                take_row(boundary[side, g * mine + k * CHUNK + i], side, i)
                return 0
            lax.fori_loop(0, CHUNK, take, 0, unroll=16)
            buf[pl.ds(pl.multiple_of(k * crows, crows), crows), :] = (
                stage[side, 0:crows, :].astype(jnp.bfloat16))
            face_copy(k, buf, dst, ss, rs, to).start()
        return 0

    lax.fori_loop(0, n_chunk, send_face, 0)

    for copy in local[5:]:
        copy.wait()

    live = counts[g, s] * EDGE_BLOCK
    slot = lax.broadcasted_iota(jnp.int32, (1, edges), 1)
    goal[...] = jnp.where(slot < live, tgt[...].reshape(1, edges), -1)
    atom = lax.broadcasted_iota(jnp.int32, (128, half), 1)

    def mark(i, _):
        at = pl.multiple_of(i * 128, 128)
        aim = jnp.broadcast_to(goal[:, pl.ds(at, 128)], (128, 128)).T
        aim = jnp.concatenate([aim] * (half // 128), axis=1)
        for k, who in enumerate((mate, g)):
            onehot[k, pl.ds(at, 128), :] = jnp.where(aim == atom + who * half, 1.0, 0.0).astype(jnp.bfloat16)
        return 0

    lax.fori_loop(0, edges // 128, mark, 0)

    def clear(i, _):
        for k in range(2):
            sums[k, pl.ds(pl.multiple_of(i * 32, 32), 32), :] = jnp.zeros((32, half), jnp.float32)
        return 0

    lax.fori_loop(0, ROWS * chan // 32, clear, 0)
    msgs[:, edges - 512:] = jnp.zeros((ROWS * chan, 512), jnp.bfloat16)

    def forward(k, buf, ss, rs):
        part = buf.at[pl.ds(pl.multiple_of((g * n_chunk + k) * crows, crows), crows), :]
        return pltpu.make_async_remote_copy(
            src_ref=part, dst_ref=part, send_sem=ss.at[k], recv_sem=rs.at[k],
            device_id=(s, mate), device_id_type=MESH)

    def widen(buf, at, base):
        table[pl.ds(base + at, crows), :] = buf[pl.ds(pl.multiple_of(at, crows), crows), :].astype(jnp.float32)

    sides = (
        (send_up, from_below, up_send, up_recv, up, fb_send, fb_recv, slab_atoms * ROWS),
        (send_down, from_above, down_send, down_recv, down, fa_send, fa_recv, (slab_atoms + face) * ROWS),
    )

    def finish_land(k, _):
        for buf, dst, ss, rs, to, fs, fr, base in sides:
            forward(k, dst, fs, fr).wait()
            widen(dst, (mate * n_chunk + k) * crows, base)
        return 0

    def land(k, _):
        for buf, dst, ss, rs, to, fs, fr, base in sides:
            face_copy(k, buf, dst, ss, rs, to).wait()
            forward(k, dst, fs, fr).start()
            widen(dst, (g * n_chunk + k) * crows, base)
        return 0

    def land_both(k, _):
        land(k, 0)
        return finish_land(k - 1, 0)

    land(0, 0)
    lax.fori_loop(1, n_chunk, land_both, 0)
    finish_land(n_chunk - 1, 0)

    G = 32
    lanes = 128
    width = 2 * lanes
    n_block = edges // width

    def gather(base, h):
        def one(i):
            return lambda: take_row(src[base + h * lanes + i], h, i)
        return [one(i) for i in range(lanes)]

    def turn(base, h):
        def one(c):
            def go():
                across[h, c] = stage[h, pl.ds(c, lanes, stride=ROWS), :].T
            return go

        def radial():
            gain[h] = rad[pl.ds(base + h * lanes, lanes), :].astype(jnp.float32).T
        return [one(c) for c in range(ROWS)] + [radial]

    def widen_rows(base, h):
        def go():
            for k in range(wig.shape[0]):
                spread[h, k] = jnp.broadcast_to(wig[k:k + 1, pl.ds(base + h * lanes, lanes)], (8, lanes))
        return [go]

    def rotate(base, h, inverse):
        at = base + h * lanes
        cols = slice(h * lanes, (h + 1) * lanes)
        steps = []
        for off, first, n in BLOCKS:

            def go(q, off, first, n):
                tops = range(q * G, (q + 1) * G, 8)
                if inverse:
                    xs = [[mixed[PLACE[first + j] * chan + t:PLACE[first + j] * chan + t + 8, cols] for t in tops]
                          for j in range(n)]
                else:
                    xs = [[across[h, first + j, t:t + 8, :] for t in tops] for j in range(n)]
                    gains = [gain[h, t:t + 8, :] for t in tops]
                for i in range(n):
                    parts = []
                    for u in range(len(tops)):
                        acc = None
                        for j in range(n):
                            term = spread[h, off + (j * n + i if inverse else i * n + j)] * xs[j][u]
                            acc = term if acc is None else acc + term
                        parts.append(acc if inverse else acc * gains[u])
                    rows = jnp.concatenate(parts, axis=0).astype(jnp.bfloat16)
                    if inverse:
                        top = (first + i) * chan + q * G
                        msgs[top:top + G, pl.ds(at, lanes)] = rows
                    else:
                        top = PLACE[first + i] * chan + q * G
                        turned[top:top + G, cols] = rows

            for q in range(chan // G):
                steps.append(functools.partial(go, q, off, first, n))
        return steps

    def mixing():
        for lo, hi, w in ((3, 7, wide_one), (0, 3, wide_zero), (7, 9, wide_two)):
            mixed[lo * chan:hi * chan, :] = jnp.dot(
                w[...], turned[lo * chan:hi * chan, :], preferred_element_type=jnp.float32)

    for h in range(2):
        weave(gather(0, h))
        weave(turn(0, h))

    span = 2 * width

    def add_up(side, pair):
        cols = pl.ds(pl.multiple_of(pair * span, span), span)

        def one(p):
            def go():
                atoms = slice(p * 256, (p + 1) * 256)
                sums[side, :, atoms] += jnp.dot(
                    msgs[:, cols], onehot[side, cols, atoms], preferred_element_type=jnp.float32)
            return go
        return [one(p) for p in range(half // 256)]

    def block(b, _):
        base = pl.multiple_of(b * width, width)
        pair = jnp.where(b < 2, n_block // 2 - 1, b // 2 - 1)
        adds = add_up(lax.rem(b, 2), pair)
        after = pl.multiple_of(jnp.where(b + 1 < n_block, b + 1, 0) * width, width)
        weave(widen_rows(base, 0))
        weave(widen_rows(base, 1))
        weave(rotate(base, 0, False), gather(after, 0), adds[0:1])
        weave(rotate(base, 1, False), gather(after, 1), turn(after, 0), adds[1:2])
        mixing()
        weave(turn(after, 1))
        weave(rotate(base, 0, True))
        weave(rotate(base, 1, True))
        return 0

    lax.fori_loop(0, n_block, block, 0)

    part = 3 * chan

    def hand_over(p):
        return pltpu.make_async_remote_copy(
            src_ref=leaving.at[p], dst_ref=arrived.at[p],
            send_sem=s_send.at[p], recv_sem=s_recv.at[p], device_id=(s, mate), device_id_type=MESH)

    last = n_block // 2 - 1
    weave(add_up(0, last))
    for p in range(3):
        leaving[p] = sums[0, p * part:(p + 1) * part, :].astype(jnp.bfloat16)
        hand_over(p).start()
    weave(add_up(1, last))
    for p in range(3):
        hand_over(p).wait()
        total = sums[1, p * part:(p + 1) * part, :] + arrived[p].astype(jnp.float32)
        total = (total * message_scale).astype(jnp.bfloat16)
        for c in range(3):
            out[3 * p + c] = total[c * chan:(c + 1) * chan, :].T


def per_device(nodes, boundary, sources, targets, block_counts, wigner, radial, w_zero, w_one, w_two):
    half, rows, chan = nodes.shape
    edges = sources.shape[0]
    face = boundary.shape[2]
    n_chunk = face // 2 // CHUNK
    atoms = 2 * half
    vm = pl.BlockSpec(memory_space=pltpu.VMEM)
    hbm = pl.BlockSpec(memory_space=pltpu.HBM)
    dma = pltpu.SemaphoreType.DMA
    out = pl.pallas_call(
        layer_kernel,
        out_shape=jax.ShapeDtypeStruct((rows, half, chan), jnp.bfloat16),
        in_specs=[hbm] * 10,
        out_specs=vm,
        scratch_shapes=[
            pltpu.SMEM((2, face), jnp.int32),
            pltpu.SMEM((edges,), jnp.int32),
            pltpu.SMEM(block_counts.shape[::-1], jnp.int32),
            pltpu.VMEM((rows, half, chan), jnp.bfloat16),
            pltpu.VMEM((edges,), jnp.int32),
            pltpu.VMEM(wigner.shape, jnp.float32),
            pltpu.VMEM(radial.shape, jnp.bfloat16),
            pltpu.VMEM(w_zero.shape, jnp.bfloat16),
            pltpu.VMEM(w_one.shape, jnp.bfloat16),
            pltpu.VMEM(w_two.shape, jnp.bfloat16),
            dma((10,)),
            pltpu.VMEM(((atoms + 2 * face) * rows, chan), jnp.float32),
            pltpu.VMEM((rows, half, chan), jnp.bfloat16),
            pltpu.VMEM((face // 2 * rows, chan), jnp.bfloat16),
            pltpu.VMEM((face // 2 * rows, chan), jnp.bfloat16),
            pltpu.VMEM((face * rows, chan), jnp.bfloat16),
            pltpu.VMEM((face * rows, chan), jnp.bfloat16),
            pltpu.VMEM((2, 128 * rows, chan), jnp.float32),
            pltpu.VMEM((2, rows, chan, 128), jnp.float32),
            pltpu.VMEM((2, chan, 128), jnp.float32),
            pltpu.VMEM((2, 35, 8, 128), jnp.float32),
            pltpu.VMEM((rows * chan, 256), jnp.bfloat16),
            pltpu.VMEM((rows * chan, 256), jnp.float32),
            pltpu.VMEM((rows * chan, edges), jnp.bfloat16),
            pltpu.VMEM((2, edges, half), jnp.bfloat16),
            pltpu.VMEM((1, edges), jnp.int32),
            pltpu.VMEM((3 * chan, 3 * chan), jnp.bfloat16),
            pltpu.VMEM((4 * chan, 4 * chan), jnp.bfloat16),
            pltpu.VMEM((2 * chan, 2 * chan), jnp.bfloat16),
            pltpu.VMEM((2, rows * chan, half), jnp.float32),
            pltpu.VMEM((3, 3 * chan, half), jnp.bfloat16),
            pltpu.VMEM((3, 3 * chan, half), jnp.bfloat16),
            dma, dma,
            dma((n_chunk,)), dma((n_chunk,)), dma((n_chunk,)), dma((n_chunk,)),
            dma((n_chunk,)), dma((n_chunk,)), dma((n_chunk,)), dma((n_chunk,)),
            dma((3,)), dma((3,)),
        ],
        compiler_params=pltpu.CompilerParams(
            collective_id=0, has_side_effects=True, vmem_limit_bytes=48 * 1024 * 1024),
        name="layer",
    )(*[pltpu.with_memory_space_constraint(a, pltpu.HBM) for a in (
        boundary[0], sources, block_counts.T, jnp.transpose(nodes, (1, 0, 2)), targets,
        wigner, radial, w_zero, w_one, w_two)])
    return jnp.transpose(out, (1, 0, 2))


def solution(mesh):
    return jax.shard_map(
        per_device,
        mesh=mesh,
        in_specs=(
            P(("slab", "graph"), None, None),
            P("slab", None, None),
            P(("slab", "graph")),
            P(("slab", "graph")),
            P(),
            P(None, ("slab", "graph")),
            P(("slab", "graph"), None),
            P(),
            P(),
            P(),
        ),
        out_specs=P(("slab", "graph"), None, None),
        check_vma=False,
    )
```

```python
import functools

import jax
import jax.numpy as jnp
from jax import lax
from jax.experimental import pallas as pl
from jax.experimental.pallas import tpu as pltpu
from jax.sharding import PartitionSpec as P

EDGE_BLOCK = 128
ROWS = 9
BLOCKS = ((0, 0, 1), (1, 1, 3), (10, 4, 5))
PLACE = {0: 0, 2: 1, 6: 2, 3: 3, 7: 4, 1: 5, 5: 6, 8: 7, 4: 8}
MESH = pl.DeviceIdType.MESH
message_scale = 0.2
CHUNK = 32


def weave(*lists):
    items = [((i + 0.5) / len(steps), k, i, step) for k, steps in enumerate(lists) for i, step in enumerate(steps)]
    for item in sorted(items, key=lambda t: t[:3]):
        item[3]()


def layer_kernel(
    boundary_hbm, src_hbm, counts_hbm, nodes_hbm, tgt_hbm, wig_hbm, rad_hbm, zero_hbm, one_hbm, two_hbm, out,
    boundary, src, counts, nodes, tgt, wig, rad, w_zero, w_one, w_two, local_sem,
    table, other, send_up, send_down, from_below, from_above, stage, across, gain, spread,
    turned, mixed, msgs, onehot, goal, wide_zero, wide_one, wide_two, sums, leaving, arrived,
    n_send, n_recv, up_send, up_recv, down_send, down_recv,
    fb_send, fb_recv, fa_send, fa_recv, s_send, s_recv,
):
    n_slab = lax.axis_size("slab")
    s = lax.axis_index("slab")
    g = lax.axis_index("graph")
    up = lax.rem(s + 1, n_slab)
    down = lax.rem(s + n_slab - 1, n_slab)
    mate = 1 - g
    half = nodes.shape[1]
    slab_atoms = 2 * half
    face = boundary.shape[1]
    mine = face // 2
    edges = src.shape[0]
    chan = nodes.shape[2]
    n_chunk = mine // CHUNK
    crows = CHUNK * ROWS

    local = [
        pltpu.make_async_copy(a, b, local_sem.at[i])
        for i, (a, b) in enumerate((
            (nodes_hbm, nodes), (boundary_hbm, boundary), (zero_hbm, w_zero), (one_hbm, w_one), (two_hbm, w_two),
            (counts_hbm, counts), (tgt_hbm, tgt), (src_hbm, src), (wig_hbm, wig), (rad_hbm, rad)))]
    for copy in local:
        copy.start()

    barrier = pltpu.get_barrier_semaphore()
    for where in ((s, mate), (up, g), (down, g)):
        pl.semaphore_signal(barrier, inc=1, device_id=where, device_id_type=MESH)
    pl.semaphore_wait(barrier, 3)

    swaps = [
        pltpu.make_async_remote_copy(
            src_ref=nodes_hbm.at[pl.ds(3 * i, 3)], dst_ref=other.at[pl.ds(3 * i, 3)],
            send_sem=n_send.at[i], recv_sem=n_recv.at[i], device_id=(s, mate), device_id_type=MESH)
        for i in range(3)]
    for swap in swaps:
        swap.start()

    def fill(planes, first, chosen):
        def step(i, _):
            at = pl.multiple_of(i * 16, 16)
            for c in chosen:
                table[pl.ds((first + at) * ROWS + c, 16, stride=ROWS), :] = (
                    planes[c, pl.ds(at, 16), :].astype(jnp.float32))
            return 0
        lax.fori_loop(0, half // 16, step, 0, unroll=2)

    local[0].wait()
    fill(nodes, g * half, range(ROWS))
    for copy in local[1:5]:
        copy.wait()

    width = w_one.shape[1]
    wide_zero[...] = w_zero[...].T
    real, imag = w_one[0].T, w_one[1].T
    wide_one[0:width, 0:width] = real
    wide_one[0:width, width:] = -imag
    wide_one[width:, 0:width] = imag
    wide_one[width:, width:] = real
    real, imag = w_two[0].T, w_two[1].T
    wide_two[0:chan, 0:chan] = real
    wide_two[0:chan, chan:] = -imag
    wide_two[chan:, 0:chan] = imag
    wide_two[chan:, chan:] = real

    for i, swap in enumerate(swaps):
        swap.wait()
        fill(other, mate * half, range(3 * i, 3 * i + 3))

    def take_row(row, h, i):
        r = row * ROWS
        stage[h, pl.ds(i * ROWS, 8), :] = table[pl.ds(r, 8), :]
        stage[h, pl.ds(i * ROWS + 8, 1), :] = table[pl.ds(r + 8, 1), :]

    def face_copy(k, buf, dst, ss, rs, to):
        return pltpu.make_async_remote_copy(
            src_ref=buf.at[pl.ds(pl.multiple_of(k * crows, crows), crows), :],
            dst_ref=dst.at[pl.ds(pl.multiple_of((g * n_chunk + k) * crows, crows), crows), :],
            send_sem=ss.at[k], recv_sem=rs.at[k], device_id=(to, g), device_id_type=MESH)

    def send_face(k, _):
        for side, buf, dst, ss, rs, to in (
            (1, send_up, from_below, up_send, up_recv, up),
            (0, send_down, from_above, down_send, down_recv, down)):
            def take(i, _):
                take_row(boundary[side, g * mine + k * CHUNK + i], side, i)
                return 0
            lax.fori_loop(0, CHUNK, take, 0, unroll=16)
            buf[pl.ds(pl.multiple_of(k * crows, crows), crows), :] = (
                stage[side, 0:crows, :].astype(jnp.bfloat16))
            face_copy(k, buf, dst, ss, rs, to).start()
        return 0

    lax.fori_loop(0, n_chunk, send_face, 0)

    for copy in local[5:]:
        copy.wait()

    live = counts[g, s] * EDGE_BLOCK
    slot = lax.broadcasted_iota(jnp.int32, (1, edges), 1)
    goal[...] = jnp.where(slot < live, tgt[...].reshape(1, edges), -1)
    atom = lax.broadcasted_iota(jnp.int32, (128, half), 1)

    def mark(i, _):
        at = pl.multiple_of(i * 128, 128)
        aim = jnp.broadcast_to(goal[:, pl.ds(at, 128)], (128, 128)).T
        aim = jnp.concatenate([aim] * (half // 128), axis=1)
        for k, who in enumerate((mate, g)):
            onehot[k, pl.ds(at, 128), :] = jnp.where(aim == atom + who * half, 1.0, 0.0).astype(jnp.bfloat16)
        return 0

    lax.fori_loop(0, edges // 128, mark, 0)

    def clear(i, _):
        for k in range(2):
            sums[k, pl.ds(pl.multiple_of(i * 32, 32), 32), :] = jnp.zeros((32, half), jnp.float32)
        return 0

    lax.fori_loop(0, ROWS * chan // 32, clear, 0)
    msgs[:, edges - 512:] = jnp.zeros((ROWS * chan, 512), jnp.bfloat16)

    def forward(k, buf, ss, rs):
        part = buf.at[pl.ds(pl.multiple_of((g * n_chunk + k) * crows, crows), crows), :]
        return pltpu.make_async_remote_copy(
            src_ref=part, dst_ref=part, send_sem=ss.at[k], recv_sem=rs.at[k],
            device_id=(s, mate), device_id_type=MESH)

    def widen(buf, at, base):
        table[pl.ds(base + at, crows), :] = buf[pl.ds(pl.multiple_of(at, crows), crows), :].astype(jnp.float32)

    sides = (
        (send_up, from_below, up_send, up_recv, up, fb_send, fb_recv, slab_atoms * ROWS),
        (send_down, from_above, down_send, down_recv, down, fa_send, fa_recv, (slab_atoms + face) * ROWS),
    )

    def finish_land(k, _):
        for buf, dst, ss, rs, to, fs, fr, base in sides:
            forward(k, dst, fs, fr).wait()
            widen(dst, (mate * n_chunk + k) * crows, base)
        return 0

    def land(k, _):
        for buf, dst, ss, rs, to, fs, fr, base in sides:
            face_copy(k, buf, dst, ss, rs, to).wait()
            forward(k, dst, fs, fr).start()
            widen(dst, (g * n_chunk + k) * crows, base)
        return 0

    def land_both(k, _):
        land(k, 0)
        return finish_land(k - 1, 0)

    land(0, 0)
    lax.fori_loop(1, n_chunk, land_both, 0)
    finish_land(n_chunk - 1, 0)

    G = 32
    lanes = 128
    width = 2 * lanes
    n_block = edges // width

    def gather(base, h):
        def one(i):
            return lambda: take_row(src[base + h * lanes + i], h, i)
        return [one(i) for i in range(lanes)]

    def turn(base, h):
        def one(c):
            def go():
                across[h, c] = stage[h, pl.ds(c, lanes, stride=ROWS), :].astype(jnp.bfloat16).T.astype(jnp.float32)
            return go

        def radial():
            gain[h] = rad[pl.ds(base + h * lanes, lanes), :].astype(jnp.float32).T
        return [one(c) for c in range(ROWS)] + [radial]

    def widen_rows(base, h):
        def go():
            for k in range(wig.shape[0]):
                spread[h, k] = jnp.broadcast_to(wig[k:k + 1, pl.ds(base + h * lanes, lanes)], (8, lanes))
        return [go]

    def rotate(base, h, inverse):
        at = base + h * lanes
        cols = slice(h * lanes, (h + 1) * lanes)
        steps = []
        for off, first, n in BLOCKS:

            def go(q, off, first, n):
                tops = range(q * G, (q + 1) * G, 8)
                if inverse:
                    xs = [[mixed[PLACE[first + j] * chan + t:PLACE[first + j] * chan + t + 8, cols] for t in tops]
                          for j in range(n)]
                else:
                    xs = [[across[h, first + j, t:t + 8, :] for t in tops] for j in range(n)]
                    gains = [gain[h, t:t + 8, :] for t in tops]
                for i in range(n):
                    parts = []
                    for u in range(len(tops)):
                        acc = None
                        for j in range(n):
                            term = spread[h, off + (j * n + i if inverse else i * n + j)] * xs[j][u]
                            acc = term if acc is None else acc + term
                        parts.append(acc if inverse else acc * gains[u])
                    rows = jnp.concatenate(parts, axis=0).astype(jnp.bfloat16)
                    if inverse:
                        top = (first + i) * chan + q * G
                        msgs[top:top + G, pl.ds(at, lanes)] = rows
                    else:
                        top = PLACE[first + i] * chan + q * G
                        turned[top:top + G, cols] = rows

            for q in range(chan // G):
                steps.append(functools.partial(go, q, off, first, n))
        return steps

    def mixing():
        for lo, hi, w in ((3, 7, wide_one), (0, 3, wide_zero), (7, 9, wide_two)):
            mixed[lo * chan:hi * chan, :] = jnp.dot(
                w[...], turned[lo * chan:hi * chan, :], preferred_element_type=jnp.float32)

    for h in range(2):
        weave(gather(0, h))
        weave(turn(0, h))

    def add_up(side, at):
        cols = pl.ds(pl.multiple_of(at, width), width)

        def one(p):
            def go():
                atoms = slice(p * 256, (p + 1) * 256)
                sums[side, :, atoms] += jnp.dot(
                    msgs[:, cols], onehot[side, cols, atoms], preferred_element_type=jnp.float32)
            return go
        return [one(p) for p in range(half // 256)]

    def block(b, _):
        base = pl.multiple_of(b * width, width)
        done = jnp.where(b < 1, n_block - 1, b - 1) * width
        adds = add_up(0, done) + add_up(1, done)
        after = pl.multiple_of(jnp.where(b + 1 < n_block, b + 1, 0) * width, width)
        weave(widen_rows(base, 0))
        weave(widen_rows(base, 1))
        weave(rotate(base, 0, False), gather(after, 0), adds[0:2])
        weave(rotate(base, 1, False), gather(after, 1), turn(after, 0), adds[2:4])
        mixing()
        weave(turn(after, 1))
        weave(rotate(base, 0, True))
        weave(rotate(base, 1, True))
        return 0

    lax.fori_loop(0, n_block, block, 0)

    part = 3 * chan

    def hand_over(p):
        return pltpu.make_async_remote_copy(
            src_ref=leaving.at[p], dst_ref=arrived.at[p],
            send_sem=s_send.at[p], recv_sem=s_recv.at[p], device_id=(s, mate), device_id_type=MESH)

    last = edges - width
    weave(add_up(0, last))
    for p in range(3):
        leaving[p] = sums[0, p * part:(p + 1) * part, :].astype(jnp.bfloat16)
        hand_over(p).start()
    weave(add_up(1, last))
    for p in range(3):
        hand_over(p).wait()
        total = sums[1, p * part:(p + 1) * part, :] + arrived[p].astype(jnp.float32)
        total = (total * message_scale).astype(jnp.bfloat16)
        for c in range(3):
            out[3 * p + c] = total[c * chan:(c + 1) * chan, :].T


def per_device(nodes, boundary, sources, targets, block_counts, wigner, radial, w_zero, w_one, w_two):
    half, rows, chan = nodes.shape
    edges = sources.shape[0]
    face = boundary.shape[2]
    n_chunk = face // 2 // CHUNK
    atoms = 2 * half
    vm = pl.BlockSpec(memory_space=pltpu.VMEM)
    hbm = pl.BlockSpec(memory_space=pltpu.HBM)
    dma = pltpu.SemaphoreType.DMA
    out = pl.pallas_call(
        layer_kernel,
        out_shape=jax.ShapeDtypeStruct((rows, half, chan), jnp.bfloat16),
        in_specs=[hbm] * 10,
        out_specs=vm,
        scratch_shapes=[
            pltpu.SMEM((2, face), jnp.int32),
            pltpu.SMEM((edges,), jnp.int32),
            pltpu.SMEM(block_counts.shape[::-1], jnp.int32),
            pltpu.VMEM((rows, half, chan), jnp.bfloat16),
            pltpu.VMEM((edges,), jnp.int32),
            pltpu.VMEM(wigner.shape, jnp.float32),
            pltpu.VMEM(radial.shape, jnp.bfloat16),
            pltpu.VMEM(w_zero.shape, jnp.bfloat16),
            pltpu.VMEM(w_one.shape, jnp.bfloat16),
            pltpu.VMEM(w_two.shape, jnp.bfloat16),
            dma((10,)),
            pltpu.VMEM(((atoms + 2 * face) * rows, chan), jnp.float32),
            pltpu.VMEM((rows, half, chan), jnp.bfloat16),
            pltpu.VMEM((face // 2 * rows, chan), jnp.bfloat16),
            pltpu.VMEM((face // 2 * rows, chan), jnp.bfloat16),
            pltpu.VMEM((face * rows, chan), jnp.bfloat16),
            pltpu.VMEM((face * rows, chan), jnp.bfloat16),
            pltpu.VMEM((2, 128 * rows, chan), jnp.float32),
            pltpu.VMEM((2, rows, chan, 128), jnp.float32),
            pltpu.VMEM((2, chan, 128), jnp.float32),
            pltpu.VMEM((2, 35, 8, 128), jnp.float32),
            pltpu.VMEM((rows * chan, 256), jnp.bfloat16),
            pltpu.VMEM((rows * chan, 256), jnp.float32),
            pltpu.VMEM((rows * chan, edges), jnp.bfloat16),
            pltpu.VMEM((2, edges, half), jnp.bfloat16),
            pltpu.VMEM((1, edges), jnp.int32),
            pltpu.VMEM((3 * chan, 3 * chan), jnp.bfloat16),
            pltpu.VMEM((4 * chan, 4 * chan), jnp.bfloat16),
            pltpu.VMEM((2 * chan, 2 * chan), jnp.bfloat16),
            pltpu.VMEM((2, rows * chan, half), jnp.float32),
            pltpu.VMEM((3, 3 * chan, half), jnp.bfloat16),
            pltpu.VMEM((3, 3 * chan, half), jnp.bfloat16),
            dma((3,)), dma((3,)),
            dma((n_chunk,)), dma((n_chunk,)), dma((n_chunk,)), dma((n_chunk,)),
            dma((n_chunk,)), dma((n_chunk,)), dma((n_chunk,)), dma((n_chunk,)),
            dma((3,)), dma((3,)),
        ],
        compiler_params=pltpu.CompilerParams(
            collective_id=0, has_side_effects=True, vmem_limit_bytes=48 * 1024 * 1024),
        name="layer",
    )(*[pltpu.with_memory_space_constraint(a, pltpu.HBM) for a in (
        boundary[0], sources, block_counts.T, jnp.transpose(nodes, (1, 0, 2)), targets,
        wigner, radial, w_zero, w_one, w_two)])
    return jnp.transpose(out, (1, 0, 2))


def solution(mesh):
    return jax.shard_map(
        per_device,
        mesh=mesh,
        in_specs=(
            P(("slab", "graph"), None, None),
            P("slab", None, None),
            P(("slab", "graph")),
            P(("slab", "graph")),
            P(),
            P(None, ("slab", "graph")),
            P(("slab", "graph"), None),
            P(),
            P(),
            P(),
        ),
        out_specs=P(("slab", "graph"), None, None),
        check_vma=False,
    )
```
